32 devices in a mesh: row: 4 (over x, core), col: 2 (over y), depth: 4 (over z).
Axes of the slice: x: 2, y: 2, z: 4, core: 2. Of those that a mesh axis runs over, the one named last changes fastest.
Arguments:
- diag_two: float32 [256, 256], replicated, may hold values from -3 to 3, as said below
- diag_one: float32 [256, 256], replicated, may hold values from -3 to 3, as said below
- cross_tile: float32 [256, 256], replicated, may hold values from -0.375 to 0.375
- left_two: float32 [256, 4096], P(None, ('col', 'depth')), may hold values from -0.375 to 0.375
- left_one: float32 [256, 4096], P(None, ('col', 'depth')), may hold values from -0.375 to 0.375
- below_left: float32 [4096, 4096], P('row', ('col', 'depth')), may hold values from -0.09375 to 0.09375
- panel_two: float32 [4096, 256], P('row', 'col'), may hold values from -0.09375 to 0.09375
- panel_one: float32 [4096, 256], P('row', 'col'), may hold values from -0.09375 to 0.09375
- grad_diag_two: float32 [256, 256], replicated, may hold values from -6 to 6
- grad_diag_one: float32 [256, 256], replicated, may hold values from -6 to 6
- grad_cross: float32 [256, 256], replicated, may hold values from -6 to 6
- grad_left_two: float32 [256, 4096], P('row', ('col', 'depth')), may hold values from -6 to 6
- grad_left_one: float32 [256, 4096], P('row', ('col', 'depth')), may hold values from -6 to 6
- grad_below: float32 [4096, 4096], P('row', ('col', 'depth')), may hold values from -6 to 6
- grad_panel_two: float32 [4096, 256], P('row', 'col'), may hold values from -6 to 6
- grad_panel_one: float32 [4096, 256], P('row', 'col'), may hold values from -6 to 6
Outputs:
- out_below: float32 [4096, 4096], P('row', ('col', 'depth'))
- out_left_two: float32 [256, 4096], P('row', ('col', 'depth'))
- out_left_one: float32 [256, 4096], P('row', ('col', 'depth'))
- out_diag_two: float32 [256, 256], replicated
- out_diag_one: float32 [256, 256], replicated
- out_cross: float32 [256, 256], replicated
- out_panel_two: float32 [4096, 256], P('row', 'col')
- out_panel_one: float32 [4096, 256], P('row', 'col')
The draws below stay inside these ranges and needn't reach their ends.
Inputs may be any that keep to these rules, and one draw needn't show every extreme that they name: `diag_two`: lower triangular; its diagonal lies in 1 to 3. `diag_one`: lower triangular; its diagonal lies in 1 to 3.
All inputs are finite; a program needn't handle non-finite values.
Results may differ from the reference program's by a relative error of at most 0.000071.
Values sent between devices are 32-bit elements; how exact they have to be, the bound alone decides.
A program may use at most 64 MiB of HBM per device.

```python
import math
import jax
import jax.numpy as jnp
from jax import lax

P_SIZE = 256
M = 4096
J = 4096


def lower_factor(key):
    first, second = jax.random.split(key)
    diagonal = jnp.exp(jax.random.uniform(first, (P_SIZE,), jnp.float32, 0.0, math.log(3.0)))
    below = jnp.clip(jax.random.normal(second, (P_SIZE, P_SIZE), jnp.float32), -5.0, 5.0) * (0.5 / math.sqrt(P_SIZE))
    return jnp.tril(below, -1) + jnp.diag(diagonal)


def draw_diag_two(key, part):
    return lower_factor(jax.random.fold_in(key, 2))


def draw_diag_one(key, part):
    return lower_factor(jax.random.fold_in(key, 1))


def steps_of(key, extent, shards, low, largest):
    loudness = 1.0
    for axis_at, parts in shards:
        heights = jax.random.uniform(jax.random.fold_in(jax.random.fold_in(key, 6), axis_at), (parts,), jnp.float32, low / len(shards), largest / len(shards))
        loudness = loudness * jnp.repeat(jnp.exp(heights), extent[axis_at] // parts).reshape((-1,) + (1,) * (len(extent) - 1 - axis_at))
    return loudness


def scatter_about(stream_key, dims, scale, limit, cuts=(), held_as=jnp.bfloat16):
    level = steps_of(stream_key, dims, cuts, -0.22, 0.18) if cuts else 1.0
    drawn = jax.random.normal(stream_key, dims, jnp.float32) * scale * level
    return jnp.minimum(jnp.maximum(drawn, -limit), limit).astype(held_as)


def setup_inputs(seed: int = 0) -> dict:
    streams_of = jax.random.split(jax.random.key(seed), 17)
    return {
        "diag_two": draw_diag_two(jax.random.fold_in(streams_of[16], 71), 0),
        "diag_one": draw_diag_one(jax.random.fold_in(streams_of[16], 71), 0),
        "cross_tile": scatter_about(streams_of[2], (P_SIZE, P_SIZE), P_SIZE ** -0.5, 0.375, (), jnp.float32),
        "left_two": scatter_about(streams_of[3], (P_SIZE, J), P_SIZE ** -0.5, 0.375, ((1, 8),), jnp.float32),
        "left_one": scatter_about(streams_of[4], (P_SIZE, J), P_SIZE ** -0.5, 0.375, ((1, 8),), jnp.float32),
        "below_left": scatter_about(streams_of[5], (M, J), M ** -0.5, 0.09375, ((0, 4), (1, 8)), jnp.float32),
        "panel_two": scatter_about(streams_of[6], (M, P_SIZE), M ** -0.5, 0.09375, ((0, 4), (1, 2)), jnp.float32),
        "panel_one": scatter_about(streams_of[7], (M, P_SIZE), M ** -0.5, 0.09375, ((0, 4), (1, 2)), jnp.float32),
        "grad_diag_two": scatter_about(streams_of[8], (P_SIZE, P_SIZE), 1.0, 6.0, (), jnp.float32),
        "grad_diag_one": scatter_about(streams_of[9], (P_SIZE, P_SIZE), 1.0, 6.0, (), jnp.float32),
        "grad_cross": scatter_about(streams_of[10], (P_SIZE, P_SIZE), 1.0, 6.0, (), jnp.float32),
        "grad_left_two": scatter_about(streams_of[11], (P_SIZE, J), 1.0, 6.0, ((0, 4), (1, 8)), jnp.float32),
        "grad_left_one": scatter_about(streams_of[12], (P_SIZE, J), 1.0, 6.0, ((0, 4), (1, 8)), jnp.float32),
        "grad_below": scatter_about(streams_of[13], (M, J), 1.0, 6.0, ((0, 4), (1, 8)), jnp.float32),
        "grad_panel_two": scatter_about(streams_of[14], (M, P_SIZE), 1.0, 6.0, ((0, 4), (1, 2)), jnp.float32),
        "grad_panel_one": scatter_about(streams_of[15], (M, P_SIZE), 1.0, 6.0, ((0, 4), (1, 2)), jnp.float32),
    }


def matmul(left, right):
    return jnp.dot(left.astype(jnp.float32), right.astype(jnp.float32), precision=lax.Precision.HIGHEST, preferred_element_type=jnp.float32)

def right_solve(factor, values):
    return lax.linalg.triangular_solve(factor, values, left_side=False, lower=True)

def halved(square):
    return jnp.tril(square) - 0.5 * jnp.diag(jnp.diag(square))

def reverse_block(factor, cotangent):
    inner = halved(matmul(factor.T, cotangent))
    leftward = lax.linalg.triangular_solve(factor, inner, left_side=True, lower=True, transpose_a=True)
    spread = right_solve(factor, leftward)
    return spread + spread.T

def reference(diag_two, diag_one, cross_tile, left_two, left_one, below_left, panel_two, panel_one, grad_diag_two, grad_diag_one, grad_cross, grad_left_two, grad_left_one, grad_below, grad_panel_two, grad_panel_one):
    solved_two = right_solve(diag_two, grad_panel_two)
    below_first = grad_below - matmul(solved_two, left_two)
    panel_next = grad_panel_one - matmul(solved_two, cross_tile)
    gram_two = matmul(solved_two.T, panel_two)
    gram_cross = matmul(solved_two.T, panel_one)
    sym_two = reverse_block(diag_two, grad_diag_two - jnp.tril(gram_two))
    cross_next = grad_cross - gram_cross - matmul(sym_two, cross_tile)
    out_cross = right_solve(diag_one, cross_next)
    out_panel_one = right_solve(diag_one, panel_next)
    out_below = below_first - matmul(out_panel_one, left_one)
    gram_one = matmul(out_cross.T, cross_tile) + matmul(out_panel_one.T, panel_one)
    sym_one = reverse_block(diag_one, grad_diag_one - jnp.tril(gram_one))
    out_left_two = grad_left_two - matmul(solved_two.T, below_left) - matmul(sym_two, left_two) - matmul(out_cross, left_one)
    out_left_one = grad_left_one - matmul(out_cross.T, left_two) - matmul(out_panel_one.T, below_left) - matmul(sym_one, left_one)
    return (out_below, out_left_two, out_left_one, halved(sym_two), halved(sym_one), out_cross, solved_two, out_panel_one)
```

```python
import jax
import jax.numpy as jnp
from jax import lax
from jax.experimental import pallas as pl
from jax.experimental.pallas import tpu as pltpu
from jax.sharding import PartitionSpec as P


def large(left, right, contract):
    return lax.dot_general(
        left,
        right,
        ((contract[:1], contract[1:]), ((), ())),
        precision=lax.Precision.HIGH,
        preferred_element_type=jnp.float32,
    )


def small(left, right, contract=(1, 0)):
    return lax.dot_general(
        left,
        right,
        ((contract[:1], contract[1:]), ((), ())),
        precision=lax.Precision.HIGHEST,
        preferred_element_type=jnp.float32,
    )


def grid_of(size):
    rows = lax.broadcasted_iota(jnp.int32, (size, size), 0)
    cols = lax.broadcasted_iota(jnp.int32, (size, size), 1)
    return rows, cols


def invert_all(blocks):
    size = blocks[0].shape[0]
    rows, cols = grid_of(size)
    apart = rows ^ cols
    lower = rows > cols
    inverses = []
    for block in blocks:
        diagonal = jnp.where(rows == cols, block, 0.0)
        down = 1.0 / jnp.sum(diagonal, axis=1, keepdims=True)
        across = 1.0 / jnp.sum(diagonal, axis=0, keepdims=True)
        pair = jnp.where(lower & (apart == 1), block, 0.0)
        inverses.append(jnp.where(rows == cols, down, 0.0) - pair * down * across)
    level = 1
    while (2 << level) <= size:
        mask = lower & ((apart >> level) == 1)
        steps = [
            small(jnp.where(mask, block, 0.0), inverse) for block, inverse in zip(blocks, inverses)
        ]
        inverses = [inverse - small(inverse, step) for inverse, step in zip(inverses, steps)]
        level += 1
    return inverses


def invert_kernel(two_ref, one_ref, cross_ref, inv_two_ref, inv_one_ref, cross_inv_ref):
    half = two_ref.shape[0] // 2
    refs = (two_ref, one_ref)
    outs = (inv_two_ref, inv_one_ref)
    blocks = []
    for ref in refs:
        blocks += [ref[:half, :half], ref[half:, half:]]
    inverses = invert_all(blocks)
    steps = [small(ref[half:, :half], inverses[2 * at]) for at, ref in enumerate(refs)]
    for at, out in enumerate(outs):
        out[:half, :half] = inverses[2 * at]
        out[half:, half:] = inverses[2 * at + 1]
        out[:half, half:] = jnp.zeros((half, half), jnp.float32)
        out[half:, :half] = -small(inverses[2 * at + 1], steps[at])
    cross_inv_ref[...] = small(cross_ref[...], inv_one_ref[...])


def chain_kernel(
    two_ref,
    one_ref,
    cross_ref,
    inv_two_ref,
    inv_one_ref,
    grad_two_ref,
    grad_one_ref,
    grad_cross_ref,
    grams_ref,
    sym_two_ref,
    sym_one_ref,
    half_two_ref,
    half_one_ref,
    out_cross_ref,
):
    size = two_ref.shape[0]
    rows, cols = grid_of(size)
    lower = rows >= cols
    scale = jnp.where(rows > cols, 1.0, jnp.where(rows == cols, 0.5, 0.0))

    def sym(factor, inverse, cotangent):
        inner = scale * small(factor, cotangent, (0, 0))
        spread = small(small(inverse, inner, (0, 0)), inverse)
        return spread + spread.T

    gram_two = grams_ref[:size, :]
    gram_cross = grams_ref[size : 2 * size, :]
    gram_below = grams_ref[2 * size :, :]
    sym_two = sym(
        two_ref[...], inv_two_ref[...], grad_two_ref[...] - jnp.where(lower, gram_two, 0.0)
    )
    sym_two_ref[...] = sym_two
    half_two_ref[...] = scale * sym_two
    cross_next = grad_cross_ref[...] - gram_cross - small(sym_two, cross_ref[...])
    out_cross = small(cross_next, inv_one_ref[...])
    out_cross_ref[...] = out_cross
    gram_one = small(out_cross, cross_ref[...], (0, 0)) + gram_below
    sym_one = sym(
        one_ref[...], inv_one_ref[...], grad_one_ref[...] - jnp.where(lower, gram_one, 0.0)
    )
    sym_one_ref[...] = sym_one
    half_one_ref[...] = scale * sym_one


def local_call(kernel, operands, count, flops):
    size = operands[0].shape[0]
    moved = 4 * size * size * (len(operands) + count)
    return pl.pallas_call(
        kernel,
        out_shape=[jax.ShapeDtypeStruct((size, size), jnp.float32)] * count,
        in_specs=[pl.BlockSpec(memory_space=pltpu.VMEM)] * len(operands),
        out_specs=[pl.BlockSpec(memory_space=pltpu.VMEM)] * count,
        cost_estimate=pl.CostEstimate(flops=flops, bytes_accessed=moved, transcendentals=0),
    )(*operands)


def swap(values, axis, bit):
    size = lax.axis_size(axis)
    return lax.ppermute(values, axis, [(at, at ^ bit) for at in range(size)])


def gathered(values, axis):
    if lax.axis_size(axis) != 2:
        return [(lax.all_gather(values, axis, axis=1, tiled=True), 0)]
    width = values.shape[1]
    at = lax.axis_index(axis)
    return [(values, at * width), (swap(values, axis, 1), (1 - at) * width)]


def times(pieces, factor):
    total = None
    for values, start in pieces:
        rows = lax.dynamic_slice_in_dim(factor, start, values.shape[1], 0)
        part = large(values, rows, (1, 0))
        total = part if total is None else total + part
    return total


def assembled(values, axis):
    size = lax.axis_size(axis)
    if size != 2:
        return lax.all_gather(values, axis, axis=1, tiled=True)
    other = swap(values, axis, 1)
    first = lax.axis_index(axis) == 0
    return jnp.concatenate(
        [jnp.where(first, values, other), jnp.where(first, other, values)], axis=1
    )


def halve(values, axis, bit):
    mine = (lax.axis_index(axis) // bit) % 2
    keep = lax.dynamic_index_in_dim(values, mine, 0, keepdims=False)
    give = lax.dynamic_index_in_dim(values, 1 - mine, 0, keepdims=False)
    return keep + swap(give, axis, bit)


def scatter_sum(values, axis):
    size = lax.axis_size(axis)
    if size & (size - 1):
        return lax.psum_scatter(values, axis, scatter_dimension=0, tiled=False)
    bit = 1
    while bit < size:
        paired = values.reshape((-1, 2) + values.shape[1:])
        values = halve(jnp.moveaxis(paired, 1, 0), axis, bit)
        bit *= 2
    return values[0]


def row_sum(values, axis, columns):
    size = lax.axis_size(axis)
    if size & (size - 1) or size < 2:
        return assembled(lax.psum(values, axis), columns)
    part = halve(values.reshape((2, -1) + values.shape[1:]), axis, 1)
    bit = 2
    while bit < size:
        part = part + swap(part, axis, bit)
        bit *= 2
    part = assembled(part, columns)
    other = swap(part, axis, 1)
    even = lax.axis_index(axis) % 2 == 0
    return jnp.concatenate([jnp.where(even, part, other), jnp.where(even, other, part)], axis=0)


def body(
    diag_two,
    diag_one,
    cross_tile,
    left_two,
    left_one,
    below_left,
    panel_two,
    panel_one,
    grad_diag_two,
    grad_diag_one,
    grad_cross,
    grad_left_two,
    grad_left_one,
    grad_below,
    grad_panel_two,
    grad_panel_one,
):
    size = diag_two.shape[0]
    share = grad_left_two.shape[0]
    width = panel_two.shape[1]
    row_start = lax.axis_index("row") * share
    col_start = lax.axis_index("col") * width
    cube = 2 * size**3

    pieces_two = gathered(grad_panel_two, "col")
    pieces_one = gathered(grad_panel_one, "col")
    inv_two, inv_one, cross_inv = local_call(
        invert_kernel, (diag_two, diag_one, cross_tile), 3, 60 * cube
    )
    solved_two = times(pieces_two, inv_two)
    solved_one = times(pieces_one, inv_one) - large(solved_two, cross_inv, (1, 0))
    partial = jnp.concatenate(
        [
            large(solved_two, panel_two, (0, 0)),
            large(solved_two, panel_one, (0, 0)),
            large(solved_one, panel_one, (0, 0)),
        ],
        axis=0,
    )
    grams = row_sum(partial, "row", "col")
    rows = lax.axis_size("row")
    lefts = jnp.stack(
        [
            large(solved_two, below_left, (0, 0)).reshape(rows, share, -1),
            large(solved_one, below_left, (0, 0)).reshape(rows, share, -1),
        ],
        axis=1,
    )
    summed = scatter_sum(lefts, "row")
    out_below = (
        grad_below - large(solved_two, left_two, (1, 0)) - large(solved_one, left_one, (1, 0))
    )
    sym_two, sym_one, half_two, half_one, out_cross = local_call(
        chain_kernel,
        (
            diag_two,
            diag_one,
            cross_tile,
            inv_two,
            inv_one,
            grad_diag_two,
            grad_diag_one,
            grad_cross,
            grams,
        ),
        5,
        60 * cube,
    )
    sym_two_rows = lax.dynamic_slice_in_dim(sym_two, row_start, share, 0)
    sym_one_rows = lax.dynamic_slice_in_dim(sym_one, row_start, share, 0)
    cross_rows = lax.dynamic_slice_in_dim(out_cross, row_start, share, 0)
    cross_cols = lax.dynamic_slice_in_dim(out_cross, row_start, share, 1)
    out_left_two = (
        grad_left_two
        - summed[0]
        - large(sym_two_rows, left_two, (1, 0))
        - large(cross_rows, left_one, (1, 0))
    )
    out_left_one = (
        grad_left_one
        - summed[1]
        - large(cross_cols, left_two, (0, 0))
        - large(sym_one_rows, left_one, (1, 0))
    )
    return (
        out_below,
        out_left_two,
        out_left_one,
        half_two,
        half_one,
        out_cross,
        lax.dynamic_slice_in_dim(solved_two, col_start, width, 1),
        lax.dynamic_slice_in_dim(solved_one, col_start, width, 1),
    )


def solution(mesh):
    panels = P("row", "col")
    lefts = P(None, ("col", "depth"))
    blocks = P("row", ("col", "depth"))
    return jax.shard_map(
        body,
        mesh=mesh,
        in_specs=(P(), P(), P(), lefts, lefts, blocks, panels, panels)
        + (P(), P(), P(), blocks, blocks, blocks, panels, panels),
        out_specs=(blocks, blocks, blocks, P(), P(), P(), panels, panels),
        check_vma=False,
    )
```

```python
import jax
import jax.numpy as jnp
from jax import lax
from jax.experimental import pallas as pl
from jax.experimental.pallas import tpu as pltpu
from jax.sharding import PartitionSpec as P


def large(left, right, contract):
    return lax.dot_general(
        left,
        right,
        ((contract[:1], contract[1:]), ((), ())),
        precision=lax.Precision.HIGH,
        preferred_element_type=jnp.float32,
    )


def small(left, right, contract=(1, 0)):
    return lax.dot_general(
        left,
        right,
        ((contract[:1], contract[1:]), ((), ())),
        precision=lax.Precision.HIGHEST,
        preferred_element_type=jnp.float32,
    )


def grid_of(size):
    rows = lax.broadcasted_iota(jnp.int32, (size, size), 0)
    cols = lax.broadcasted_iota(jnp.int32, (size, size), 1)
    return rows, cols


def invert_all(blocks):
    size = blocks[0].shape[0]
    rows, cols = grid_of(size)
    apart = rows ^ cols
    lower = rows > cols
    inverses = []
    for block in blocks:
        diagonal = jnp.where(rows == cols, block, 0.0)
        down = 1.0 / jnp.sum(diagonal, axis=1, keepdims=True)
        across = 1.0 / jnp.sum(diagonal, axis=0, keepdims=True)
        pair = jnp.where(lower & (apart == 1), block, 0.0)
        inverses.append(jnp.where(rows == cols, down, 0.0) - pair * down * across)
    level = 1
    while (2 << level) <= size:
        mask = lower & ((apart >> level) == 1)
        steps = [
            small(jnp.where(mask, block, 0.0), inverse) for block, inverse in zip(blocks, inverses)
        ]
        inverses = [inverse - small(inverse, step) for inverse, step in zip(inverses, steps)]
        level += 1
    return inverses


def invert_kernel(two_ref, one_ref, cross_ref, inv_two_ref, inv_one_ref, cross_inv_ref):
    half = two_ref.shape[0] // 2
    refs = (two_ref, one_ref)
    outs = (inv_two_ref, inv_one_ref)
    blocks = []
    for ref in refs:
        blocks += [ref[:half, :half], ref[half:, half:]]
    inverses = invert_all(blocks)
    steps = [small(ref[half:, :half], inverses[2 * at]) for at, ref in enumerate(refs)]
    for at, out in enumerate(outs):
        out[:half, :half] = inverses[2 * at]
        out[half:, half:] = inverses[2 * at + 1]
        out[:half, half:] = jnp.zeros((half, half), jnp.float32)
        out[half:, :half] = -small(inverses[2 * at + 1], steps[at])
    cross_inv_ref[...] = small(cross_ref[...], inv_one_ref[...])


def chain_kernel(
    two_ref,
    one_ref,
    cross_ref,
    inv_two_ref,
    inv_one_ref,
    grad_two_ref,
    grad_one_ref,
    grad_cross_ref,
    place_ref,
    *rest,
):
    grams, outs = rest[:-5], rest[-5:]
    chain(
        two_ref,
        one_ref,
        cross_ref,
        inv_two_ref,
        inv_one_ref,
        grad_two_ref,
        grad_one_ref,
        grad_cross_ref,
        joined(grams, place_ref),
        *outs,
    )


def joined(grams, place_ref):
    if len(grams) == 1:
        return grams[0][...]
    mine, beside, twin, across = [gram[...] for gram in grams]
    left = place_ref[0] == 0
    upper = place_ref[1] == 0
    own = jnp.concatenate([jnp.where(left, mine, beside), jnp.where(left, beside, mine)], axis=1)
    far = jnp.concatenate([jnp.where(left, twin, across), jnp.where(left, across, twin)], axis=1)
    return jnp.concatenate([jnp.where(upper, own, far), jnp.where(upper, far, own)], axis=0)


def chain(
    two_ref,
    one_ref,
    cross_ref,
    inv_two_ref,
    inv_one_ref,
    grad_two_ref,
    grad_one_ref,
    grad_cross_ref,
    grams,
    sym_two_ref,
    sym_one_ref,
    half_two_ref,
    half_one_ref,
    out_cross_ref,
):
    size = two_ref.shape[0]
    rows, cols = grid_of(size)
    lower = rows >= cols
    scale = jnp.where(rows > cols, 1.0, jnp.where(rows == cols, 0.5, 0.0))

    def sym(factor, inverse, cotangent):
        inner = scale * small(factor, cotangent, (0, 0))
        spread = small(small(inverse, inner, (0, 0)), inverse)
        return spread + spread.T

    gram_two = grams[:size, :]
    gram_cross = grams[size : 2 * size, :]
    gram_below = grams[2 * size :, :]
    sym_two = sym(
        two_ref[...], inv_two_ref[...], grad_two_ref[...] - jnp.where(lower, gram_two, 0.0)
    )
    sym_two_ref[...] = sym_two
    half_two_ref[...] = scale * sym_two
    cross_next = grad_cross_ref[...] - gram_cross - small(sym_two, cross_ref[...])
    out_cross = small(cross_next, inv_one_ref[...])
    out_cross_ref[...] = out_cross
    gram_one = small(out_cross, cross_ref[...], (0, 0)) + gram_below
    sym_one = sym(
        one_ref[...], inv_one_ref[...], grad_one_ref[...] - jnp.where(lower, gram_one, 0.0)
    )
    sym_one_ref[...] = sym_one
    half_one_ref[...] = scale * sym_one


def local_call(kernel, operands, count, flops):
    size = operands[0].shape[0]
    moved = 4 * size * size * (len(operands) + count)
    return pl.pallas_call(
        kernel,
        out_shape=[jax.ShapeDtypeStruct((size, size), jnp.float32)] * count,
        in_specs=[
            pl.BlockSpec(memory_space=pltpu.SMEM if operand.ndim == 1 else pltpu.VMEM)
            for operand in operands
        ],
        out_specs=[pl.BlockSpec(memory_space=pltpu.VMEM)] * count,
        cost_estimate=pl.CostEstimate(flops=flops, bytes_accessed=moved, transcendentals=0),
    )(*operands)


def swap(values, axis, bit):
    size = lax.axis_size(axis)
    return lax.ppermute(values, axis, [(at, at ^ bit) for at in range(size)])


def gathered(values, axis):
    if lax.axis_size(axis) != 2:
        return [(lax.all_gather(values, axis, axis=1, tiled=True), 0)]
    width = values.shape[1]
    at = lax.axis_index(axis)
    return [(values, at * width), (swap(values, axis, 1), (1 - at) * width)]


def parted(values):
    high = values.astype(jnp.bfloat16)
    return high, (values - high.astype(jnp.float32)).astype(jnp.bfloat16)


def product(left, right):
    (left_high, left_low), (right_high, right_low) = parted(left), parted(right)

    def single(one, other):
        return jnp.dot(one, other, preferred_element_type=jnp.float32)

    return (single(left_low, right_high) + single(left_high, right_low)) + single(
        left_high, right_high
    )


def solve_kernel(count, starts_ref, inverse_ref, *refs):
    pieces, extra, outs = refs[:count], refs[count:-count], refs[-count:]
    total = None
    for at, piece in enumerate(pieces):
        width = piece.shape[1]
        rows = inverse_ref[pl.ds(pl.multiple_of(starts_ref[at], width), width), :]
        part = product(piece[...], rows)
        total = part if total is None else total + part
    if extra:
        total = total - product(extra[0][...], extra[1][...])
    outs[0][...] = total
    if count > 1:
        width = outs[1].shape[1]
        outs[1][...] = jnp.where(starts_ref[0] == 0, total[:, :width], total[:, width:])


def solve(pieces, inverse, *extra):
    count = len(pieces)
    rows, width = pieces[0][0].shape
    size = inverse.shape[0]
    block = rows // 4
    starts = jnp.stack([jnp.asarray(start, jnp.int32) for _, start in pieces])

    def tall(columns):
        return pl.BlockSpec((block, columns), lambda step: (step, 0))

    whole = pl.BlockSpec((size, size), lambda step: (0, 0))
    widths = [size, width][:count]
    return pl.pallas_call(
        lambda *refs: solve_kernel(count, *refs),
        grid=(4,),
        out_shape=[jax.ShapeDtypeStruct((rows, columns), jnp.float32) for columns in widths],
        in_specs=[pl.BlockSpec(memory_space=pltpu.SMEM), whole]
        + [tall(values.shape[1]) for values, _ in pieces]
        + ([tall(size), whole] if extra else []),
        out_specs=[tall(columns) for columns in widths],
        cost_estimate=pl.CostEstimate(
            flops=6 * rows * size * size, bytes_accessed=12 * rows * size, transcendentals=0
        ),
    )(starts, inverse, *[values for values, _ in pieces], *extra)


def assembled(values, axis):
    size = lax.axis_size(axis)
    if size != 2:
        return lax.all_gather(values, axis, axis=1, tiled=True)
    other = swap(values, axis, 1)
    first = lax.axis_index(axis) == 0
    return jnp.concatenate(
        [jnp.where(first, values, other), jnp.where(first, other, values)], axis=1
    )


def halve(values, axis, bit):
    mine = (lax.axis_index(axis) // bit) % 2
    keep = lax.dynamic_index_in_dim(values, mine, 0, keepdims=False)
    give = lax.dynamic_index_in_dim(values, 1 - mine, 0, keepdims=False)
    return keep + swap(give, axis, bit)


def scatter_sum(values, axis):
    size = lax.axis_size(axis)
    if size & (size - 1):
        return lax.psum_scatter(values, axis, scatter_dimension=0, tiled=False)
    bit = 1
    while bit < size:
        paired = values.reshape((-1, 2) + values.shape[1:])
        values = halve(jnp.moveaxis(paired, 1, 0), axis, bit)
        bit *= 2
    return values[0]


def row_sum(values, axis, columns):
    size = lax.axis_size(axis)
    if size & (size - 1) or size < 2:
        return [assembled(lax.psum(values, axis), columns)]
    part = halve(values.reshape((2, -1) + values.shape[1:]), axis, 1)
    bit = 2
    while bit < size:
        part = part + swap(part, axis, bit)
        bit *= 2
    if lax.axis_size(columns) == 2:
        beside = swap(part, columns, 1)
        return [part, beside, swap(part, axis, 1), swap(beside, axis, 1)]
    part = assembled(part, columns)
    other = swap(part, axis, 1)
    even = lax.axis_index(axis) % 2 == 0
    return [jnp.concatenate([jnp.where(even, part, other), jnp.where(even, other, part)], axis=0)]


def body(
    diag_two,
    diag_one,
    cross_tile,
    left_two,
    left_one,
    below_left,
    panel_two,
    panel_one,
    grad_diag_two,
    grad_diag_one,
    grad_cross,
    grad_left_two,
    grad_left_one,
    grad_below,
    grad_panel_two,
    grad_panel_one,
):
    size = diag_two.shape[0]
    share = grad_left_two.shape[0]
    width = panel_two.shape[1]
    row_start = lax.axis_index("row") * share
    col_start = lax.axis_index("col") * width
    cube = 2 * size**3

    pieces_two = gathered(grad_panel_two, "col")
    pieces_one = gathered(grad_panel_one, "col")
    inv_two, inv_one, cross_inv = local_call(
        invert_kernel, (diag_two, diag_one, cross_tile), 3, 60 * cube
    )
    solved_two, *own_two = solve(pieces_two, inv_two)
    solved_one, *own_one = solve(pieces_one, inv_one, solved_two, cross_inv)
    place = jnp.stack([lax.axis_index("col"), lax.axis_index("row") % 2]).astype(jnp.int32)
    partial = jnp.concatenate(
        [
            large(solved_two, panel_two, (0, 0)),
            large(solved_two, panel_one, (0, 0)),
            large(solved_one, panel_one, (0, 0)),
        ],
        axis=0,
    )
    grams = row_sum(partial, "row", "col")
    rows = lax.axis_size("row")
    lefts = jnp.stack(
        [
            large(solved_two, below_left, (0, 0)).reshape(rows, share, -1),
            large(solved_one, below_left, (0, 0)).reshape(rows, share, -1),
        ],
        axis=1,
    )
    summed = scatter_sum(lefts, "row")
    out_below = (
        grad_below - large(solved_two, left_two, (1, 0)) - large(solved_one, left_one, (1, 0))
    )
    sym_two, sym_one, half_two, half_one, out_cross = local_call(
        chain_kernel,
        (
            diag_two,
            diag_one,
            cross_tile,
            inv_two,
            inv_one,
            grad_diag_two,
            grad_diag_one,
            grad_cross,
            place,
            *grams,
        ),
        5,
        60 * cube,
    )
    sym_two_rows = lax.dynamic_slice_in_dim(sym_two, row_start, share, 0)
    sym_one_rows = lax.dynamic_slice_in_dim(sym_one, row_start, share, 0)
    cross_rows = lax.dynamic_slice_in_dim(out_cross, row_start, share, 0)
    cross_cols = lax.dynamic_slice_in_dim(out_cross, row_start, share, 1)
    out_left_two = (
        grad_left_two
        - summed[0]
        - large(sym_two_rows, left_two, (1, 0))
        - large(cross_rows, left_one, (1, 0))
    )
    out_left_one = (
        grad_left_one
        - summed[1]
        - large(cross_cols, left_two, (0, 0))
        - large(sym_one_rows, left_one, (1, 0))
    )
    return (
        out_below,
        out_left_two,
        out_left_one,
        half_two,
        half_one,
        out_cross,
        own_two[0] if own_two else lax.dynamic_slice_in_dim(solved_two, col_start, width, 1),
        own_one[0] if own_one else lax.dynamic_slice_in_dim(solved_one, col_start, width, 1),
    )


def solution(mesh):
    panels = P("row", "col")
    lefts = P(None, ("col", "depth"))
    blocks = P("row", ("col", "depth"))
    return jax.shard_map(
        body,
        mesh=mesh,
        in_specs=(P(), P(), P(), lefts, lefts, blocks, panels, panels)
        + (P(), P(), P(), blocks, blocks, blocks, panels, panels),
        out_specs=(blocks, blocks, blocks, P(), P(), P(), panels, panels),
        check_vma=False,
    )
```
